32 devices in a mesh: irrep: 4 (over z), occ: 4 (over y, core), vir: 2 (over x).
Axes of the slice: x: 2, y: 2, z: 4, core: 2. Of those that a mesh axis runs over, the one named last changes fastest.
Arguments:
- amplitudes: bfloat16 [8, 320, 12288], P('irrep', None, ('occ', 'vir')), may hold values from -6 to 6
- ladder_ints: bfloat16 [8, 12288, 12288], P('irrep', ('occ', 'vir')), may hold values from -0.078125 to 0.078125
- hole_ints: bfloat16 [8, 320, 320], P('irrep'), may hold values from -0.3125 to 0.3125
- occ_energy: float32 [8, 320], P('irrep'), may hold values from -3 to -0.5
- vir_energy: float32 [8, 12288], P('irrep', ('occ', 'vir')), may hold values from 0.5 to 3
- occ_pairs: int32 [8], replicated, may hold values from 160 to 320, as said below
- vir_pairs: int32 [8], replicated, may hold values from 6144 to 12288, as said below
Outputs:
- updated: bfloat16 [8, 320, 12288], P('irrep', None, ('occ', 'vir'))
- residual_norm: float32 [8], P('irrep')
The draws below stay inside these ranges and needn't reach their ends.
Inputs may be any that keep to these rules, and one draw needn't show every extreme that they name: `occ_pairs`: some block has exactly 320 live occupied pairs in every draw. `vir_pairs`: some block has exactly 12288 live virtual pairs in every draw.
All inputs are finite; a program needn't handle non-finite values.
Results may differ from the reference program's by a relative error of at most 0.001.
Values may be sent and summed in bfloat16 or wider, within the bound.
No kernel may reach another device: no remote copies, remote signals or barrier semaphores. Data moves between devices by JAX's collectives and lax.ppermute only.
A program may use at most 192 MiB of HBM per device.

```python
import jax
import jax.numpy as jnp

NB = 8
OP = 320
VP = 12288


def draw_occ_pairs(key, part):
    first_key, second_key = jax.random.split(jax.random.fold_in(key, 11))
    values = jax.random.randint(first_key, (NB,), OP // 2, OP + 1)
    chosen = jax.random.randint(second_key, (), 0, NB)
    return jnp.where(jnp.arange(NB) == chosen, OP, values).astype(jnp.int32)


def draw_vir_pairs(key, part):
    first_key, second_key = jax.random.split(jax.random.fold_in(key, 23))
    values = jax.random.randint(first_key, (NB,), VP // 2, VP + 1)
    chosen = jax.random.randint(second_key, (), 0, NB)
    return jnp.where(jnp.arange(NB) == chosen, VP, values).astype(jnp.int32)


def with_spikes(drawn, stream_key, source, target, shards_of, factor):
    def block_of(dim):
        return (jnp.arange(drawn.shape[dim]) // (drawn.shape[dim] // shards_of)).reshape((-1,) + (1,) * (drawn.ndim - 1 - dim))

    near = jax.random.permutation(stream_key, shards_of)[block_of(target)]
    second = (block_of(target) + shards_of // 2) % shards_of
    return jnp.where((block_of(source) == near) | (block_of(source) == second), factor * drawn, drawn)


def shard_levels(stream_key, shape, pieces, low, largest):
    def one(position, blocks):
        steps = jax.random.uniform(jax.random.fold_in(jax.random.fold_in(stream_key, 6), position), (blocks,), jnp.float32, low / len(pieces), largest / len(pieces))
        return jnp.repeat(jnp.exp(steps), shape[position] // blocks).reshape((-1,) + (1,) * (len(shape) - position - 1))

    gain = one(*pieces[0])
    for cut in pieces[1:]:
        gain = gain * one(*cut)
    return gain


def centred(stream_key, dims, scale, bound, cuts=(), kind=jnp.bfloat16):
    gain = shard_levels(stream_key, dims, cuts, -0.22, 0.18) if cuts else 1.0
    result = jax.random.normal(stream_key, dims, jnp.float32) * scale * gain
    return jnp.minimum(jnp.maximum(result, -bound), bound).astype(kind)


def heavy_noise(own_key, shape, deviation, bound, shards, heavy, kind=jnp.bfloat16):
    entries = deviation * jax.random.normal(own_key, shape, jnp.float32)
    if shards:
        entries = entries * shard_levels(own_key, shape, shards, -0.22, 0.18)
    return jnp.clip(with_spikes(entries, jax.random.fold_in(own_key, 3), *heavy), -bound, bound).astype(kind)


def setup_inputs(seed: int = 0) -> dict:
    splits = jax.random.split(jax.random.key(seed), 8)
    amplitudes = centred(splits[0], (NB, OP, VP), 1.0, 6.0, ((0, 4), (2, 8)))
    ladder_ints = heavy_noise(splits[1], (NB, VP, VP), VP ** -0.5, 0.078125, ((0, 4), (1, 8)), (1, 2, 8, 2.0))
    hole_ints = centred(splits[2], (NB, OP, OP), OP ** -0.5, 0.3125, ((0, 4),))
    occ_energy = jnp.clip(-3.0 + 2.5 * jax.random.uniform(splits[3], (NB, OP), jnp.float32) ** shard_levels(splits[3], (NB, OP), ((0, 4),), -0.2, 0.2), -3.0, -0.5)
    vir_energy = jnp.clip(0.5 + 2.5 * jax.random.uniform(splits[4], (NB, VP), jnp.float32) ** shard_levels(splits[4], (NB, VP), ((0, 4), (1, 8)), -0.2, 0.2), 0.5, 3.0)
    occ_pairs = draw_occ_pairs(jax.random.fold_in(splits[7], 71), 0)
    vir_pairs = draw_vir_pairs(jax.random.fold_in(splits[7], 71), 0)
    return dict(amplitudes=amplitudes, ladder_ints=ladder_ints, hole_ints=hole_ints, occ_energy=occ_energy, vir_energy=vir_energy, occ_pairs=occ_pairs, vir_pairs=vir_pairs)


LEVEL_SHIFT = 0.5
EPSILON = 1e-06

def reference(amplitudes, ladder_ints, hole_ints, occ_energy, vir_energy, occ_pairs, vir_pairs):
    row_index = jnp.arange(OP, dtype=jnp.int32)
    col_index = jnp.arange(VP, dtype=jnp.int32)
    results = []
    norms = []
    for block in range(NB):
        keep_mask = (row_index[:, None] < occ_pairs[block]) & (col_index[None, :] < vir_pairs[block])
        masked = jnp.where(keep_mask, amplitudes[block], jnp.zeros((), amplitudes.dtype))
        ladder_term = jnp.dot(masked, ladder_ints[block], preferred_element_type=jnp.float32)
        hole_term = jnp.dot(hole_ints[block], masked, preferred_element_type=jnp.float32)
        wide = masked.astype(jnp.float32)
        denominator = vir_energy[block][None, :] - occ_energy[block][:, None]
        residual = jnp.where(keep_mask, ladder_term + hole_term + denominator * wide, jnp.zeros((), jnp.float32))
        updated = wide - residual / (denominator + LEVEL_SHIFT)
        pair_count = (occ_pairs[block] * vir_pairs[block]).astype(jnp.float32)
        results.append(updated.astype(jnp.bfloat16))
        norms.append(jnp.sqrt(jnp.sum(residual * residual) / pair_count + EPSILON))
    return (jnp.stack(results), jnp.stack(norms))
```

```python
import functools

import jax
import jax.numpy as jnp
from jax import lax
from jax.experimental import pallas as pl
from jax.experimental.pallas import tpu as pltpu
from jax.sharding import PartitionSpec as P

LEVEL_SHIFT = 0.5
EPSILON = 1e-06
GROUP = ("occ", "vir")
LANES = 128
CODE_ROWS = 8
CODE_STEPS = 256.0
TOP = 32766.0


def table_lookup(table, block_ids):
    entries = table.shape[0]
    match = jnp.arange(entries, dtype=jnp.int32)[None, :] == block_ids[:, None]
    return jnp.sum(jnp.where(match, table[None, :], 0), axis=1)


def stage_bits(mesh):
    devices = mesh.devices.reshape(mesh.shape["irrep"], -1)[0]
    count = len(devices).bit_length() - 1
    bits = list(range(count))

    def same_chip(bit):
        first, second = devices[0], devices[1 << bit]
        where = getattr(first, "coords", None)
        return where is not None and where == getattr(second, "coords", None)

    near = [b for b in bits if same_chip(b)]
    return near + [b for b in bits if b not in near]


def chunk_plan(width):
    if width % (6 * LANES) == 0:
        unit = width // 6
        return [(unit, 2), (3 * unit, 1), (2 * unit, 0)]
    if width % (3 * LANES) == 0:
        unit = width // 3
        return [(unit, 2), (2 * unit, 0)]
    return [(width, 0)]


def packet_rows(rows, width):
    return (width // LANES) * (rows // 2) + CODE_ROWS


def unpack_add(total, packet, rows, width):
    half = rows // 2
    tiles = width // LANES
    out = []
    for t in range(tiles):
        words = packet[t * half : (t + 1) * half, :]
        code = packet[tiles * half + t : tiles * half + t + 1, :]
        scale = jnp.exp2(code.astype(jnp.float32) * (1.0 / CODE_STEPS)) * (1.0 / TOP)
        high = lax.shift_right_arithmetic(words, 16).astype(jnp.float32) * scale
        low = lax.shift_right_arithmetic(lax.shift_left(words, 16), 16).astype(jnp.float32) * scale
        a, b = total[t]
        out.append((a + high, b + low))
    return out


def pack_into(out_ref, total, rows, width):
    half = rows // 2
    tiles = width // LANES
    code_row = lax.broadcasted_iota(jnp.int32, (CODE_ROWS, LANES), 0)
    codes = jnp.zeros((CODE_ROWS, LANES), jnp.int32)
    for t in range(tiles):
        a, b = total[t]
        peak = jnp.max(jnp.maximum(jnp.abs(a), jnp.abs(b)), axis=0, keepdims=True)
        level = jnp.ceil(jnp.log2(jnp.maximum(peak, 1e-30)) * CODE_STEPS) + 1.0
        code = level.astype(jnp.int32)
        factor = jnp.exp2(level * (-1.0 / CODE_STEPS)) * TOP
        high = jnp.round(a * factor).astype(jnp.int32)
        low = jnp.round(b * factor).astype(jnp.int32)
        out_ref[t * half : (t + 1) * half, :] = lax.shift_left(high, 16) | (low & 0xFFFF)
        codes = jnp.where(code_row == t, code, codes)
    out_ref[tiles * half : tiles * half + CODE_ROWS, :] = codes


def lane_tiles(acc_ref, rows, width):
    half = rows // 2
    return [
        (acc_ref[:half, t * LANES : (t + 1) * LANES], acc_ref[half:, t * LANES : (t + 1) * LANES])
        for t in range(width // LANES)
    ]


def send_kernel(plan, block_count, recv_count, rows, width, *refs):
    prefetch, refs = refs[:1], refs[1:]
    t_ref, v_ref, refs = refs[0], refs[1], refs[2:]
    recv_refs, refs = refs[: block_count * recv_count], refs[block_count * recv_count :]
    out_refs, (acc_ref,) = refs[:block_count], refs[block_count:]
    block = pl.program_id(0)
    acc_ref[...] = jnp.dot(t_ref[...], v_ref[...], preferred_element_type=jnp.float32)
    for h in range(block_count):

        @pl.when(block == h)
        def _():
            total = lane_tiles(acc_ref, rows, width)
            for r in range(recv_count):
                total = unpack_add(total, recv_refs[h * recv_count + r][...], rows, width)
            pack_into(out_refs[h], total, rows, width)


def held_index(h, picks, count):
    def index(block, item, table):
        del table
        here = picks[0] + 0 * item
        for i in range(1, count):
            here = jnp.where(item == i, picks[i], here)
        here = jnp.where(block < h, picks[0], jnp.where(block > h, picks[count - 1], here))
        return (here, 0, 0)

    return index


def send_call(masked, ladder_ints, slot, masks, recvs, width, place):
    block_count, rows, depth = masked.shape
    per_segment = depth // width
    count = len(masks[0])
    table = jnp.stack([(slot ^ jnp.asarray(m, jnp.int32)) * per_segment + place for m in masks])
    recv_count = len(recvs[0])
    length = packet_rows(rows, width)
    in_specs = [
        pl.BlockSpec((None, rows, depth), lambda block, item, table: (block, 0, 0)),
        pl.BlockSpec((None, depth, width), lambda block, item, table: (block, 0, table[block, item])),
    ]
    operands = [masked, ladder_ints]
    for h in range(block_count):
        for packet, picks in recvs[h]:
            in_specs.append(pl.BlockSpec((None, length, LANES), held_index(h, picks, count)))
            operands.append(packet)
    out_specs = [
        pl.BlockSpec((None, length, LANES), held_index(h, list(range(count)), count)) for h in range(block_count)
    ]
    out_shape = [jax.ShapeDtypeStruct((count, length, LANES), jnp.int32) for _ in range(block_count)]
    steps = block_count * count
    cost = pl.CostEstimate(
        flops=2 * steps * rows * depth * width,
        bytes_accessed=steps * (2 * depth * width + (1 + recv_count) * length * LANES * 4) + 2 * masked.size,
        transcendentals=0,
    )
    return pl.pallas_call(
        functools.partial(send_kernel, None, block_count, recv_count, rows, width),
        grid_spec=pltpu.PrefetchScalarGridSpec(
            num_scalar_prefetch=1,
            grid=(block_count, count),
            in_specs=in_specs,
            out_specs=out_specs,
            scratch_shapes=[pltpu.VMEM((rows, width), jnp.float32)],
        ),
        out_shape=out_shape,
        cost_estimate=cost,
        compiler_params=pltpu.CompilerParams(dimension_semantics=("arbitrary", "arbitrary")),
        name=f"send{recv_count}_{width}",
    )(table, *operands)


def last_kernel(block_count, recv_count, rows, width, place, *refs):
    (limits,), refs = refs[:1], refs[1:]
    t_ref, v_ref, here_ref, hole_ref, occ_ref, vir_ref, refs = *refs[:6], refs[6:]
    recv_refs, refs = refs[: block_count * recv_count], refs[block_count * recv_count :]
    out_ref, sum_ref, acc_ref = refs
    block = pl.program_id(0)
    here = here_ref[...]
    acc_ref[...] = jnp.dot(t_ref[...], v_ref[...], preferred_element_type=jnp.float32) + jnp.dot(
        hole_ref[...], here, preferred_element_type=jnp.float32
    )
    for h in range(block_count):

        @pl.when(block == h)
        def _():
            half = rows // 2
            total = lane_tiles(acc_ref, rows, width)
            for r in range(recv_count):
                total = unpack_add(total, recv_refs[h * recv_count + r][...], rows, width)
            occ_live, vir_live = limits[0, h], limits[1, h] - limits[2, 0] - place * width
            squares = jnp.zeros((CODE_ROWS, LANES), jnp.float32)
            for t in range(width // LANES):
                cols = slice(t * LANES, (t + 1) * LANES)
                col_index = lax.broadcasted_iota(jnp.int32, (half, LANES), 1) + t * LANES
                row_index = lax.broadcasted_iota(jnp.int32, (half, LANES), 0)
                for part in range(2):
                    span = slice(part * half, (part + 1) * half)
                    keep = (row_index + part * half < occ_live) & (col_index < vir_live)
                    wide = here_ref[span, cols].astype(jnp.float32)
                    denominator = vir_ref[:, cols] - occ_ref[span, :]
                    residual = jnp.where(keep, total[t][part] + denominator * wide, 0.0)
                    out_ref[span, cols] = (wide - residual / (denominator + LEVEL_SHIFT)).astype(jnp.bfloat16)
                    squares += jnp.sum((residual * residual).reshape(-1, CODE_ROWS, LANES), axis=0)
            sum_ref[...] = squares


def last_call(masked, ladder_ints, hole_ints, occ_column, vir_row, slot, limits, recvs, width, place):
    block_count, rows, depth = masked.shape
    per_segment = depth // width
    recv_count = len(recvs[0])
    length = packet_rows(rows, width)
    table = jnp.concatenate([limits, jnp.full((1, block_count), slot * depth), jnp.full((1, block_count), slot)])
    in_specs = [
        pl.BlockSpec((None, rows, depth), lambda block, table: (block, 0, 0)),
        pl.BlockSpec((None, depth, width), lambda block, table: (block, 0, table[3, 0] * per_segment + place)),
        pl.BlockSpec((None, rows, width), lambda block, table: (block, 0, place)),
        pl.BlockSpec((None, rows, rows), lambda block, table: (block, 0, 0)),
        pl.BlockSpec((None, rows, 1), lambda block, table: (block, 0, 0)),
        pl.BlockSpec((None, 1, width), lambda block, table: (block, 0, place)),
    ]
    operands = [masked, ladder_ints, masked, hole_ints, occ_column, vir_row]
    for h in range(block_count):
        for packet, picks in recvs[h]:
            in_specs.append(pl.BlockSpec((None, length, LANES), lambda block, table, pick=picks[0]: (pick, 0, 0)))
            operands.append(packet)
    cost = pl.CostEstimate(
        flops=2 * block_count * rows * (depth + rows) * width,
        bytes_accessed=block_count * (2 * depth * width + recv_count * length * LANES * 4 + 2 * rows * depth),
        transcendentals=0,
    )
    return pl.pallas_call(
        functools.partial(last_kernel, block_count, recv_count, rows, width, place),
        grid_spec=pltpu.PrefetchScalarGridSpec(
            num_scalar_prefetch=1,
            grid=(block_count,),
            in_specs=in_specs,
            out_specs=[
                pl.BlockSpec((None, rows, width), lambda block, table: (block, 0, 0)),
                pl.BlockSpec((None, CODE_ROWS, LANES), lambda block, table: (block, 0, 0)),
            ],
            scratch_shapes=[pltpu.VMEM((rows, width), jnp.float32)],
        ),
        out_shape=[
            jax.ShapeDtypeStruct((block_count, rows, width), jnp.bfloat16),
            jax.ShapeDtypeStruct((block_count, CODE_ROWS, LANES), jnp.float32),
        ],
        cost_estimate=cost,
        compiler_params=pltpu.CompilerParams(dimension_semantics=("arbitrary",)),
        name=f"last_{width}",
    )(table, *operands)


def patterns(bits):
    found = [0]
    for b in bits:
        found = found + [m | (1 << b) for m in found]
    return found


def body(order, amplitudes, ladder_ints, hole_ints, occ_energy, vir_energy, occ_pairs, vir_pairs):
    block_count, pair_rows, cols_here = amplitudes.shape
    vir_devices = lax.axis_size("vir")
    devices = lax.axis_size(GROUP)
    block_ids = lax.axis_index("irrep") * block_count + jnp.arange(block_count, dtype=jnp.int32)
    slot = lax.axis_index("occ") * vir_devices + lax.axis_index("vir")
    occ_here = table_lookup(occ_pairs, block_ids)
    vir_here = table_lookup(vir_pairs, block_ids)
    row_index = jnp.arange(pair_rows, dtype=jnp.int32)
    col_index = slot * cols_here + jnp.arange(cols_here, dtype=jnp.int32)
    keep_mask = (row_index[None, :, None] < occ_here[:, None, None]) & (
        col_index[None, None, :] < vir_here[:, None, None]
    )
    masked = jnp.where(keep_mask, amplitudes, jnp.zeros((), amplitudes.dtype))
    limits = jnp.stack([occ_here, vir_here])
    occ_column = occ_energy[:, :, None]
    vir_row = vir_energy[:, None, :]

    def swap(packet, bit):
        pairs = [(d, d ^ (1 << bit)) for d in range(devices)]
        return lax.ppermute(packet, GROUP, pairs)

    orders = [order if h % 2 == 0 else order[:1] + order[:0:-1] for h in range(block_count)]
    blocks = range(block_count)
    chunks = chunk_plan(cols_here)
    stages = len(order)
    pieces, sums = [None] * len(chunks), []
    for width, place in chunks:
        held = [[] for _ in blocks]

        def picked(masks):
            return [[(p, [had.index(m) for m in masks[h]]) for p, had in held[h] if masks[h][0] in had] for h in blocks]

        first = [[patterns(o[2:]) for o in orders]]
        near = [[m | (1 << o[1]) for m in p] for o, p in zip(orders, first[0])]
        for wanted in (near, first[0]):
            masks = [[m | (1 << o[0]) for m in w] for o, w in zip(orders, wanted)]
            packets = send_call(masked, ladder_ints, slot, masks, [[] for _ in blocks], width, place)
            for h in blocks:
                held[h].append((swap(packets[h], orders[h][0]), wanted[h]))
        for t in range(1, stages):
            masks = [[m | (1 << o[t]) for m in patterns(o[t + 1 :])] for o in orders]
            packets = send_call(masked, ladder_ints, slot, masks, picked(masks), width, place)
            for h in blocks:
                held[h].append((swap(packets[h], orders[h][t]), patterns(orders[h][t + 1 :])))
        piece, squares = last_call(
            masked, ladder_ints, hole_ints, occ_column, vir_row, slot, limits,
            picked([[0] for _ in blocks]), width, place,
        )
        pieces[chunks.index((width, place))] = (place * width, piece)
        sums.append(squares)
    updated = jnp.concatenate([p for _, p in sorted(pieces, key=lambda e: e[0])], axis=2)
    squares = jnp.sum(functools.reduce(jnp.add, sums), axis=(1, 2))
    for bit in order:
        squares = squares + swap(squares, bit)
    pair_count = (occ_here * vir_here).astype(jnp.float32)
    residual_norm = jnp.sqrt(squares / pair_count + EPSILON)
    return (updated, residual_norm)


def solution(mesh):
    in_specs = (
        P("irrep", None, ("occ", "vir")),
        P("irrep", ("occ", "vir"), None),
        P("irrep", None, None),
        P("irrep", None),
        P("irrep", ("occ", "vir")),
        P(),
        P(),
    )
    out_specs = (P("irrep", None, ("occ", "vir")), P("irrep"))
    return jax.shard_map(
        functools.partial(body, stage_bits(mesh)),
        mesh=mesh,
        in_specs=in_specs,
        out_specs=out_specs,
        check_vma=False,
    )
```

```python
import functools

import jax
import jax.numpy as jnp
from jax import lax
from jax.experimental import pallas as pl
from jax.experimental.pallas import tpu as pltpu
from jax.sharding import PartitionSpec as P


LEVEL_SHIFT = 0.5
EPSILON = 1e-06
GROUP = ("occ", "vir")
LANES = 128
CODE_ROWS = 8
CODE_STEPS = 256.0
TOP = 32766.0
VMEM_LIMIT = 6 * 1024 * 1024
IN_VMEM = pl.BlockSpec(memory_space=pltpu.VMEM)
IN_HBM = pl.BlockSpec(memory_space=pltpu.HBM)
IN_SMEM = pl.BlockSpec(memory_space=pltpu.SMEM)


def stage_bits(mesh):
    devices = mesh.devices.reshape(mesh.shape["irrep"], -1)[0]
    bits = list(range(len(devices).bit_length() - 1))

    def same_chip(bit):
        where = getattr(devices[0], "coords", None)
        return where is not None and where == getattr(devices[1 << bit], "coords", None)

    near = [b for b in bits if same_chip(b)]
    return near + [b for b in bits if b not in near]


def turn_plan(width, order):
    other = order[:1] + order[:0:-1]
    if width % (6 * LANES) == 0:
        unit = width // 6
        return [
            (unit, 0, [order]),
            (unit, unit, [other]),
            (unit, 2 * unit, [order, other]),
            (unit, 4 * unit, [order, other]),
        ]
    for turns in (4, 3, 2):
        if width % (turns * LANES) == 0:
            unit = width // turns
            return [(unit, n * unit, [other if n % 2 else order]) for n in range(turns)]
    return [(width, 0, [order])]


def patterns(bits):
    found = [0]
    for b in bits:
        found = found + [m | (1 << b) for m in found]
    return found


def packet_shape(count, rows, width):
    tiles = count * (width // LANES)
    return (tiles * (rows // 2) + pl.cdiv(tiles, CODE_ROWS) * CODE_ROWS, LANES)


def row_of(table, n):
    here = lax.broadcasted_iota(jnp.int32, table.shape, 0) == n
    return jnp.sum(jnp.where(here, table, jnp.zeros_like(table)), axis=0, keepdims=True)


def unpack_add(total, packet, count, piece, rows, width):
    half = rows // 2
    tiles = width // LANES
    base = count * tiles * half
    out = []
    for t in range(tiles):
        n = piece * tiles + t
        codes = packet[pl.ds(pl.multiple_of(base + n // CODE_ROWS * CODE_ROWS, CODE_ROWS), CODE_ROWS), :]
        scales = jnp.exp2(codes.astype(jnp.float32) * (1.0 / CODE_STEPS)) * (1.0 / TOP)
        scale = row_of(scales, n % CODE_ROWS)
        words = packet[pl.ds(pl.multiple_of(n * half, CODE_ROWS), half), :]
        high = lax.shift_right_arithmetic(words, 16).astype(jnp.float32) * scale
        low = lax.shift_right_arithmetic(lax.shift_left(words, 16), 16).astype(jnp.float32) * scale
        a, b = total[t]
        out.append((a + high, b + low))
    return out


def pack_into(packet, total, count, piece, rows, width):
    half = rows // 2
    tiles = width // LANES
    base = count * tiles * half
    for t in range(tiles):
        n = piece * tiles + t
        a, b = total[t]
        peak = jnp.max(jnp.maximum(jnp.abs(a), jnp.abs(b)), axis=0, keepdims=True)
        level = jnp.ceil(jnp.log2(jnp.maximum(peak, 1e-30)) * CODE_STEPS) + 1.0
        factor = jnp.exp2(level * (-1.0 / CODE_STEPS)) * TOP
        high = jnp.round(a * factor).astype(jnp.int32)
        low = jnp.round(b * factor).astype(jnp.int32)
        packet[pl.ds(pl.multiple_of(n * half, CODE_ROWS), half), :] = lax.shift_left(high, 16) | (low & 0xFFFF)
        place = pl.ds(pl.multiple_of(base + n // CODE_ROWS * CODE_ROWS, CODE_ROWS), CODE_ROWS)
        here = lax.broadcasted_iota(jnp.int32, (CODE_ROWS, LANES), 0) == n % CODE_ROWS
        packet[place, :] = jnp.where(here, level.astype(jnp.int32), packet[place, :])


def lane_tiles(acc, rows, width):
    half = rows // 2
    return [
        (acc[:half, t * LANES : (t + 1) * LANES], acc[half:, t * LANES : (t + 1) * LANES])
        for t in range(width // LANES)
    ]


def my_slot():
    return lax.axis_index("occ") * lax.axis_size("vir") + lax.axis_index("vir")


def fetch(source, target, sems, block, spots, depth, width, n):
    mask, place = spots[n]
    first = (my_slot() ^ mask) * depth + place
    return pltpu.make_async_copy(
        source.at[block, :, pl.ds(pl.multiple_of(first, width), width)],
        target.at[block, n],
        sems.at[block, n],
    )


def fetch_all(source, target, sems, blocks, spots, depth, width, verb):
    for h in range(blocks):
        for n in range(len(spots)):
            getattr(fetch(source, target, sems, h, spots, depth, width, n), verb)()


def open_kernel(spots, width, source, pieces, sems):
    blocks, depth, _ = source.shape
    fetch_all(source, pieces, sems, blocks, spots, depth, width, "start")
    fetch_all(source, pieces, sems, blocks, spots, depth, width, "wait")


def open_call(ladder_ints, turn):
    block_count, depth, _ = ladder_ints.shape
    width, spots = turn
    return pl.pallas_call(
        functools.partial(open_kernel, spots, width),
        in_specs=[IN_HBM],
        out_specs=IN_VMEM,
        scratch_shapes=[pltpu.SemaphoreType.DMA((block_count, len(spots)))],
        out_shape=pltpu.VMEM((block_count, len(spots), depth, width), ladder_ints.dtype),
        compiler_params=pltpu.CompilerParams(vmem_limit_bytes=VMEM_LIMIT),
        name="open",
    )(ladder_ints)


def send_kernel(cfg, *refs):
    parts, count, first_col, recv_picks, own_picks, rows, width, _, next_width, next_spots, masking = cfg
    refs = list(refs)
    take = lambda n: [refs.pop(0) for _ in range(n)]
    own = own_picks is not None
    t_ref, source = take(2)
    occ_ref, vir_ref = take(2) if masking else (None, None)
    (pieces,) = take(1)
    recv_refs = [take(len(picks)) for picks in recv_picks]
    (hole_ref,) = take(1) if own else (None,)
    own_refs = [take(len(picks)) for picks in own_picks] if own else []
    out_refs = take(parts)
    (own_out,) = take(1) if own else (None,)
    (masked_ref,) = take(1) if masking else (None,)
    (next_pieces,) = take(1) if next_spots else (None,)
    blocks, _, depth = t_ref.shape

    if next_spots:
        (next_sems,) = take(1)
        fetch_all(source, next_pieces, next_sems, blocks, next_spots, depth, next_width, "start")
    half = rows // 2

    def step(block, carry):
        if masking:
            block_id = lax.axis_index("irrep") * blocks + block
            row_index = lax.broadcasted_iota(jnp.int32, (rows, depth), 0)
            col_index = lax.broadcasted_iota(jnp.int32, (rows, depth), 1)
            keep = (row_index < occ_ref[block_id]) & (col_index < vir_ref[block_id] - my_slot() * depth)
            masked_ref[block] = jnp.where(keep, t_ref[block].astype(jnp.float32), 0.0).astype(masked_ref.dtype)
        held_ref = masked_ref if masking else t_ref
        left = held_ref[block]

        def product(n):
            return jnp.dot(left, pieces[block, n], preferred_element_type=jnp.float32)

        for i in range(count):
            for c in range(parts):
                total = lane_tiles(product(i * parts + c), rows, width)
                for ref, (held, picks) in zip(recv_refs[c], recv_picks[c]):
                    total = unpack_add(total, ref, blocks * held, block * held + picks[i], rows, width)
                pack_into(out_refs[c], total, blocks * count, block * count + i, rows, width)
        if own:
            for c in range(parts):
                first = first_col + c * width
                acc = product(count * parts + c) + jnp.dot(
                    hole_ref[block], held_ref[block, :, first : first + width], preferred_element_type=jnp.float32
                )
                total = lane_tiles(acc, rows, width)
                for ref, (held, picks) in zip(own_refs[c], own_picks[c]):
                    total = unpack_add(total, ref, blocks * held, block * held + picks[0], rows, width)
                for t, (a, b) in enumerate(total):
                    cols = slice(c * width + t * LANES, c * width + (t + 1) * LANES)
                    own_out[block, :half, cols] = a
                    own_out[block, half:, cols] = b
        return carry

    lax.fori_loop(0, blocks, step, 0)
    if next_spots:
        fetch_all(source, next_pieces, next_sems, blocks, next_spots, depth, next_width, "wait")


def picks_of(recvs, wanted):
    return [(len(held), [held.index(m) for m in wanted]) for _, held in recvs]


def spots_of(width, first_col, masks, own):
    parts = len(masks)
    spots = [(masks[c][i], first_col + c * width) for i in range(len(masks[0])) for c in range(parts)]
    return spots + ([(0, first_col + c * width) for c in range(parts)] if own else [])


def send_call(t, ladder_ints, live, width, first_col, masks, recvs, own, pieces, next_turn):
    block_count, rows, depth = t.shape
    parts, count = len(masks), len(masks[0])
    both = parts * width
    masking = live is not None
    spots = spots_of(width, first_col, masks, own is not None)
    next_width, next_spots = next_turn
    in_specs, operands = [IN_VMEM, IN_HBM], [t, ladder_ints]
    if masking:
        in_specs += [IN_SMEM, IN_SMEM]
        operands += live
    in_specs.append(IN_VMEM)
    operands.append(pieces)
    for c in range(parts):
        in_specs += [IN_VMEM] * len(recvs[c])
        operands += [array for array, _ in recvs[c]]
    packet = pltpu.VMEM(packet_shape(block_count * count, rows, width), jnp.int32)
    out_shape = [packet] * parts
    own_picks = None
    if own is not None:
        hole_ints, own_recvs = own
        own_picks = [picks_of(r, [0]) for r in own_recvs]
        in_specs.append(IN_VMEM)
        operands.append(hole_ints)
        for c in range(parts):
            in_specs += [IN_VMEM] * len(own_recvs[c])
            operands += [array for array, _ in own_recvs[c]]
        out_shape.append(pltpu.VMEM((block_count, rows, both), jnp.float32))
    scratch = []
    if masking:
        out_shape.append(pltpu.VMEM(t.shape, t.dtype))
    if next_spots:
        out_shape.append(pltpu.VMEM((block_count, len(next_spots), depth, next_width), ladder_ints.dtype))
        scratch.append(pltpu.SemaphoreType.DMA((block_count, len(next_spots))))
    steps = block_count * len(spots)
    cost = pl.CostEstimate(
        flops=2 * steps * rows * depth * width, bytes_accessed=steps * 2 * depth * width, transcendentals=0
    )
    recv_picks = [picks_of(r, m) for r, m in zip(recvs, masks)]
    cfg = (parts, count, first_col, recv_picks, own_picks, rows, width, spots, next_width, next_spots, masking)
    return pl.pallas_call(
        functools.partial(send_kernel, cfg),
        in_specs=in_specs,
        out_specs=[IN_VMEM] * len(out_shape),
        scratch_shapes=scratch,
        out_shape=out_shape,
        cost_estimate=cost,
        compiler_params=pltpu.CompilerParams(vmem_limit_bytes=VMEM_LIMIT),
    )(*operands)


def finish_kernel(cfg, *refs):
    parts, rows, width, start, first_turn, want_update, want_squares, with_alias = cfg
    refs = list(refs)
    take = lambda n: [refs.pop(0) for _ in range(n)]
    own_ref, t_ref, occ_ref, vir_ref, occ_live_ref, vir_live_ref = take(6)
    recv_refs = take(parts)
    take(with_alias)
    (out_ref,) = take(1) if want_update else (None,)
    (sum_ref,) = take(1) if want_squares else (None,)
    block = pl.program_id(0)
    blocks, _, depth = t_ref.shape
    half = rows // 2
    tiles = width // LANES
    if first_turn:
        (column_ref,) = take(1)
        for r in range(0, rows, CODE_ROWS * 5):
            size = min(CODE_ROWS * 5, rows - r)
            row_index = lax.broadcasted_iota(jnp.int32, (size, rows), 0) + r
            col_index = lax.broadcasted_iota(jnp.int32, (size, rows), 1)
            occ = occ_ref[0:1, :]
            for h in range(1, blocks):
                occ = jnp.where(block == h, occ_ref[h : h + 1, :], occ)
            column = jnp.sum(jnp.where(row_index == col_index, occ, 0.0), axis=1, keepdims=True)
            column_ref[block, r : r + size, :] = jnp.broadcast_to(column, (size, LANES))
    else:
        column_ref = occ_ref
    block_id = lax.axis_index("irrep") * blocks + block
    occ_live = occ_live_ref[block_id]
    vir_live = vir_live_ref[block_id] - my_slot() * depth - start
    squares = jnp.zeros((CODE_ROWS, LANES), jnp.float32)
    row_index = lax.broadcasted_iota(jnp.int32, (half, LANES), 0)
    lane_index = lax.broadcasted_iota(jnp.int32, (half, LANES), 1)
    spans = [slice(0, half), slice(half, rows)]
    for c in range(parts):
        firsts = [c * width + t * LANES for t in range(tiles)]
        total = [tuple(own_ref[block, span, first : first + LANES] for span in spans) for first in firsts]
        total = unpack_add(total, recv_refs[c], blocks, block, rows, width)
        for t, first in enumerate(firsts):
            cols = slice(first, first + LANES)
            here = slice(start + first, start + first + LANES)
            vir = vir_ref[0:1, here]
            for h in range(1, blocks):
                vir = jnp.where(block == h, vir_ref[h : h + 1, here], vir)
            for part, span in enumerate(spans):
                keep = (row_index + part * half < occ_live) & (lane_index + first < vir_live)
                wide = t_ref[block, span, here].astype(jnp.float32)
                denominator = vir - column_ref[block, span, :]
                residual = jnp.where(keep, total[t][part] + denominator * wide, 0.0)
                if want_update:
                    out_ref[span, cols] = (wide - residual / (denominator + LEVEL_SHIFT)).astype(jnp.bfloat16)
                if want_squares:
                    squares += jnp.sum((residual * residual).reshape(-1, CODE_ROWS, LANES), axis=0)
    if want_squares:
        pair_count = jnp.full(squares.shape, occ_live * vir_live_ref[block_id], jnp.int32)
        sum_ref[...] = squares / pair_count.astype(jnp.float32)


def finish_call(t_masked, own, occ, vir_energy, live, width, start, recvs, updated, want_update, want_squares):
    block_count, rows, depth = t_masked.shape
    parts = len(recvs)
    both = parts * width
    first_turn = occ.ndim == 2
    operands = [own, t_masked, occ, vir_energy, *live] + [array for array, _ in recvs]
    in_specs = [IN_VMEM] * 4 + [IN_SMEM] * 2 + [IN_VMEM] * parts
    aliases = {}
    with_alias = int(want_update and updated is not None)
    if with_alias:
        in_specs.append(IN_HBM)
        operands.append(updated)
        aliases = {len(operands) - 1: 0}
    out_specs, out_shape = [], []
    if want_update:
        out_specs.append(pl.BlockSpec((None, rows, both), lambda h: (h, 0, start // both)))
        out_shape.append(jax.ShapeDtypeStruct((block_count, rows, depth), jnp.bfloat16))
    if want_squares:
        out_specs.append(pl.BlockSpec((None, CODE_ROWS, LANES), lambda h: (h, 0, 0)))
        out_shape.append(jax.ShapeDtypeStruct((block_count, CODE_ROWS, LANES), jnp.float32))
    if first_turn:
        out_specs.append(IN_VMEM)
        out_shape.append(jax.ShapeDtypeStruct((block_count, rows, LANES), jnp.float32))
    cfg = (parts, rows, width, start, first_turn, want_update, want_squares, with_alias)
    return pl.pallas_call(
        functools.partial(finish_kernel, cfg),
        grid=(block_count,),
        in_specs=in_specs,
        out_specs=out_specs,
        out_shape=out_shape,
        input_output_aliases=aliases,
        cost_estimate=pl.CostEstimate(
            flops=60 * block_count * rows * both, bytes_accessed=10 * block_count * rows * both, transcendentals=0
        ),
        compiler_params=pltpu.CompilerParams(dimension_semantics=("arbitrary",), vmem_limit_bytes=VMEM_LIMIT),
    )(*operands)


def job_order(turns, stages):
    jobs, far = [], []
    singles = turns[:2] if len(turns) > 2 else turns[:1]
    jobs += [(n, 0, True) for n in singles] + [(n, 1, None) for n in singles]
    far += list(singles)
    for n in turns[len(singles) :]:
        jobs += [(n, 0, True), (far.pop(0), 0, False), (n, 1, None)]
        far.append(n)
    if stages == 3 and len(turns) > 2:
        jobs += [(n, 2, None) for n in singles] + [(n, 0, False) for n in far]
        return jobs + [(n, 2, None) for n in turns[len(singles) :]]
    jobs += [(n, 0, False) for n in far]
    return jobs + [(n, t, None) for t in range(2, stages) for n in turns]


def body(order, *arrays):
    return residual_step(order, *arrays)


def residual_step(order, amplitudes, ladder_ints, hole_ints, occ_energy, vir_energy, occ_pairs, vir_pairs):
    _, _, cols_here = amplitudes.shape
    devices = lax.axis_size(GROUP)
    live = [occ_pairs, vir_pairs]

    def swap(packet, mask):
        return lax.ppermute(packet, GROUP, [(d, d ^ mask) for d in range(devices)])

    stages = len(order)
    plan = turn_plan(cols_here, order)
    turns = list(range(len(plan)))
    held = [[[] for _ in orders] for _, _, orders in plan]

    def having(turn, masks):
        return [[p for p in had if m[0] in p[1]] for had, m in zip(held[turn], masks)]

    calls = []
    for turn, t, near in job_order(turns, stages):
        orders = plan[turn][2]
        wanted = [patterns(o[2:] if t == 0 else o[t + 1 :]) for o in orders]
        if near:
            wanted = [[m | (1 << o[1]) for m in w] for o, w in zip(orders, wanted)]
        calls.append((turn, t, wanted, [[m | (1 << o[t]) for m in w] for o, w in zip(orders, wanted)]))
    spots = [
        (plan[turn][0], spots_of(plan[turn][0], plan[turn][1], masks, t == stages - 1)) for turn, t, _, masks in calls
    ] + [(0, None)]
    t_here, owns = amplitudes, {}
    pieces = open_call(ladder_ints, spots[0])
    for n, (turn, t, wanted, masks) in enumerate(calls):
        width, start, orders = plan[turn]
        parts = len(orders)
        own = (hole_ints, having(turn, [[0]] * parts)) if t == stages - 1 else None
        outs = send_call(
            t_here, ladder_ints, None if n else live, width, start, masks, having(turn, masks), own, pieces,
            spots[n + 1],
        )
        if own is not None:
            owns[turn] = outs[parts]
        if n == 0:
            t_here = outs[parts]
        if spots[n + 1][1]:
            pieces = outs[-1]
        for c, o in enumerate(orders):
            packet = outs[c]
            if t == stages - 1 and turn == turns[-1] - 1:
                packet = lax.optimization_barrier((packet, held[turns[-1]][0][-1][0]))[0]
            held[turn][c].append((swap(packet, 1 << o[t]), wanted[c]))
    updated, sums, occ = None, [], occ_energy
    for turn in turns:
        width, start, _ = plan[turn]

        def finish(want_update, want_squares):
            return finish_call(
                t_here, owns[turn], occ, vir_energy, live, width, start, [h[-1] for h in held[turn]], updated,
                want_update, want_squares,
            )

        if turn == turns[-1] and turn:
            (squares,) = finish(False, True)
            (updated,) = finish(True, False)
        else:
            updated, squares, *rest = finish(True, True)
            occ = rest[0] if rest else occ
        sums.append(squares)
    squares = jnp.sum(functools.reduce(jnp.add, sums), axis=(1, 2))
    squares = squares + swap(squares, 1 << order[0])
    across = []
    for mask in patterns(order[1:])[1:]:
        across.append(swap(squares, mask))
    residual_norm = jnp.sqrt(functools.reduce(jnp.add, [squares] + across) + EPSILON)
    return (updated, residual_norm)


def solution(mesh):
    in_specs = (
        P("irrep", None, ("occ", "vir")),
        P("irrep", ("occ", "vir"), None),
        P("irrep", None, None),
        P("irrep", None),
        P("irrep", ("occ", "vir")),
        P(),
        P(),
    )
    out_specs = (P("irrep", None, ("occ", "vir")), P("irrep"))
    order = stage_bits(mesh)
    return jax.shard_map(
        functools.partial(body, order), mesh=mesh, in_specs=in_specs, out_specs=out_specs, check_vma=False
    )
```

```python
import functools

import jax
import jax.numpy as jnp
from jax import lax
from jax.experimental import pallas as pl
from jax.experimental.pallas import tpu as pltpu
from jax.sharding import PartitionSpec as P


LEVEL_SHIFT = 0.5
EPSILON = 1e-06
GROUP = ("occ", "vir")
LANES = 128
CODE_ROWS = 8
CODE_STEPS = 256.0
TOP = 32766.0
VMEM_LIMIT = 6 * 1024 * 1024
IN_VMEM = pl.BlockSpec(memory_space=pltpu.VMEM)
IN_HBM = pl.BlockSpec(memory_space=pltpu.HBM)
IN_SMEM = pl.BlockSpec(memory_space=pltpu.SMEM)


def stage_bits(mesh):
    devices = mesh.devices.reshape(mesh.shape["irrep"], -1)[0]
    bits = list(range(len(devices).bit_length() - 1))

    def same_chip(bit):
        where = getattr(devices[0], "coords", None)
        return where is not None and where == getattr(devices[1 << bit], "coords", None)

    near = [b for b in bits if same_chip(b)]
    return near + [b for b in bits if b not in near]


def turn_plan(width, order):
    other = order[:1] + order[:0:-1]
    if width % (6 * LANES) == 0:
        unit = width // 6
        return [
            (unit, 0, [order]),
            (unit, unit, [other]),
            (unit, 2 * unit, [order, other]),
            (unit, 4 * unit, [order, other]),
        ]
    for turns in (4, 3, 2):
        if width % (turns * LANES) == 0:
            unit = width // turns
            return [(unit, n * unit, [other if n % 2 else order]) for n in range(turns)]
    return [(width, 0, [order])]


def patterns(bits):
    found = [0]
    for b in bits:
        found = found + [m | (1 << b) for m in found]
    return found


def packet_shape(count, rows, width):
    tiles = count * (width // LANES)
    return (tiles * (rows // 2) + pl.cdiv(tiles, CODE_ROWS) * CODE_ROWS, LANES)


def row_of(table, n):
    here = lax.broadcasted_iota(jnp.int32, table.shape, 0) == n
    return jnp.sum(jnp.where(here, table, jnp.zeros_like(table)), axis=0, keepdims=True)


def unpack_add(total, packet, count, piece, rows, width):
    half = rows // 2
    tiles = width // LANES
    base = count * tiles * half
    out = []
    for t in range(tiles):
        n = piece * tiles + t
        codes = packet[pl.ds(pl.multiple_of(base + n // CODE_ROWS * CODE_ROWS, CODE_ROWS), CODE_ROWS), :]
        scales = jnp.exp2(codes.astype(jnp.float32) * (1.0 / CODE_STEPS)) * (1.0 / TOP)
        scale = row_of(scales, n % CODE_ROWS)
        words = packet[pl.ds(pl.multiple_of(n * half, CODE_ROWS), half), :]
        high = lax.shift_right_arithmetic(words, 16).astype(jnp.float32) * scale
        low = lax.shift_right_arithmetic(lax.shift_left(words, 16), 16).astype(jnp.float32) * scale
        a, b = total[t]
        out.append((a + high, b + low))
    return out


def pack_into(packet, total, count, piece, rows, width):
    half = rows // 2
    tiles = width // LANES
    base = count * tiles * half
    for t in range(tiles):
        n = piece * tiles + t
        a, b = total[t]
        peak = jnp.max(jnp.maximum(jnp.abs(a), jnp.abs(b)), axis=0, keepdims=True)
        level = jnp.ceil(jnp.log2(jnp.maximum(peak, 1e-30)) * CODE_STEPS) + 1.0
        factor = jnp.exp2(level * (-1.0 / CODE_STEPS)) * TOP
        high = jnp.round(a * factor).astype(jnp.int32)
        low = jnp.round(b * factor).astype(jnp.int32)
        packet[pl.ds(pl.multiple_of(n * half, CODE_ROWS), half), :] = lax.shift_left(high, 16) | (low & 0xFFFF)
        place = pl.ds(pl.multiple_of(base + n // CODE_ROWS * CODE_ROWS, CODE_ROWS), CODE_ROWS)
        here = lax.broadcasted_iota(jnp.int32, (CODE_ROWS, LANES), 0) == n % CODE_ROWS
        packet[place, :] = jnp.where(here, level.astype(jnp.int32), packet[place, :])


def lane_tiles(acc, rows, width):
    half = rows // 2
    return [
        (acc[:half, t * LANES : (t + 1) * LANES], acc[half:, t * LANES : (t + 1) * LANES])
        for t in range(width // LANES)
    ]


def my_slot():
    return lax.axis_index("occ") * lax.axis_size("vir") + lax.axis_index("vir")


def fetch(source, target, sems, block, spots, depth, width, n):
    mask, place = spots[n]
    first = (my_slot() ^ mask) * depth + place
    return pltpu.make_async_copy(
        source.at[block, :, pl.ds(pl.multiple_of(first, width), width)],
        target.at[block, n],
        sems.at[block, n],
    )


def fetch_all(source, target, sems, blocks, spots, depth, width, verb):
    for h in range(blocks):
        for n in range(len(spots)):
            getattr(fetch(source, target, sems, h, spots, depth, width, n), verb)()


def open_kernel(spots, width, source, pieces, sems):
    blocks, depth, _ = source.shape
    fetch_all(source, pieces, sems, blocks, spots, depth, width, "start")
    fetch_all(source, pieces, sems, blocks, spots, depth, width, "wait")


def open_call(ladder_ints, turn):
    block_count, depth, _ = ladder_ints.shape
    width, spots = turn
    return pl.pallas_call(
        functools.partial(open_kernel, spots, width),
        in_specs=[IN_HBM],
        out_specs=IN_VMEM,
        scratch_shapes=[pltpu.SemaphoreType.DMA((block_count, len(spots)))],
        out_shape=pltpu.VMEM((block_count, len(spots), depth, width), ladder_ints.dtype),
        compiler_params=pltpu.CompilerParams(vmem_limit_bytes=VMEM_LIMIT),
        name="open",
    )(ladder_ints)


def send_kernel(cfg, *refs):
    parts, count, first_col, recv_picks, own_picks, rows, width, _, next_width, next_spots, masking = cfg
    refs = list(refs)
    take = lambda n: [refs.pop(0) for _ in range(n)]
    own = own_picks is not None
    t_ref, source = take(2)
    occ_ref, vir_ref = take(2) if masking else (None, None)
    (pieces,) = take(1)
    recv_refs = [take(len(picks)) for picks in recv_picks]
    (hole_ref,) = take(1) if own else (None,)
    own_refs = [take(len(picks)) for picks in own_picks] if own else []
    out_refs = take(parts)
    (own_out,) = take(1) if own else (None,)
    (masked_ref,) = take(1) if masking else (None,)
    (next_pieces,) = take(1) if next_spots else (None,)
    blocks, _, depth = t_ref.shape

    if next_spots:
        (next_sems,) = take(1)
        fetch_all(source, next_pieces, next_sems, blocks, next_spots, depth, next_width, "start")
    half = rows // 2

    def step(block, carry):
        if masking:
            block_id = lax.axis_index("irrep") * blocks + block
            row_index = lax.broadcasted_iota(jnp.int32, (rows, depth), 0)
            col_index = lax.broadcasted_iota(jnp.int32, (rows, depth), 1)
            keep = (row_index < occ_ref[block_id]) & (col_index < vir_ref[block_id] - my_slot() * depth)
            masked_ref[block] = jnp.where(keep, t_ref[block].astype(jnp.float32), 0.0).astype(masked_ref.dtype)
        held_ref = masked_ref if masking else t_ref
        left = held_ref[block]

        def product(n):
            return jnp.dot(left, pieces[block, n], preferred_element_type=jnp.float32)

        for i in range(count):
            for c in range(parts):
                total = lane_tiles(product(i * parts + c), rows, width)
                for ref, (held, picks) in zip(recv_refs[c], recv_picks[c]):
                    total = unpack_add(total, ref, blocks * held, block * held + picks[i], rows, width)
                pack_into(out_refs[c], total, blocks * count, block * count + i, rows, width)
        if own:
            for c in range(parts):
                first = first_col + c * width
                acc = product(count * parts + c) + jnp.dot(
                    hole_ref[block], held_ref[block, :, first : first + width], preferred_element_type=jnp.float32
                )
                total = lane_tiles(acc, rows, width)
                for ref, (held, picks) in zip(own_refs[c], own_picks[c]):
                    total = unpack_add(total, ref, blocks * held, block * held + picks[0], rows, width)
                for t, (a, b) in enumerate(total):
                    cols = slice(c * width + t * LANES, c * width + (t + 1) * LANES)
                    own_out[block, :half, cols] = a
                    own_out[block, half:, cols] = b
        return carry

    lax.fori_loop(0, blocks, step, 0)
    if next_spots:
        fetch_all(source, next_pieces, next_sems, blocks, next_spots, depth, next_width, "wait")


def picks_of(recvs, wanted):
    return [(len(held), [held.index(m) for m in wanted]) for _, held in recvs]


def spots_of(width, first_col, masks, own):
    parts = len(masks)
    spots = [(masks[c][i], first_col + c * width) for i in range(len(masks[0])) for c in range(parts)]
    return spots + ([(0, first_col + c * width) for c in range(parts)] if own else [])


def send_call(t, ladder_ints, live, width, first_col, masks, recvs, own, pieces, next_turn):
    block_count, rows, depth = t.shape
    parts, count = len(masks), len(masks[0])
    both = parts * width
    masking = live is not None
    spots = spots_of(width, first_col, masks, own is not None)
    next_width, next_spots = next_turn
    in_specs, operands = [IN_VMEM, IN_HBM], [t, ladder_ints]
    if masking:
        in_specs += [IN_SMEM, IN_SMEM]
        operands += live
    in_specs.append(IN_VMEM)
    operands.append(pieces)
    for c in range(parts):
        in_specs += [IN_VMEM] * len(recvs[c])
        operands += [array for array, _ in recvs[c]]
    packet = pltpu.VMEM(packet_shape(block_count * count, rows, width), jnp.int32)
    out_shape = [packet] * parts
    own_picks = None
    if own is not None:
        hole_ints, own_recvs = own
        own_picks = [picks_of(r, [0]) for r in own_recvs]
        in_specs.append(IN_VMEM)
        operands.append(hole_ints)
        for c in range(parts):
            in_specs += [IN_VMEM] * len(own_recvs[c])
            operands += [array for array, _ in own_recvs[c]]
        out_shape.append(pltpu.VMEM((block_count, rows, both), jnp.float32))
    scratch = []
    if masking:
        out_shape.append(pltpu.VMEM(t.shape, t.dtype))
    if next_spots:
        out_shape.append(pltpu.VMEM((block_count, len(next_spots), depth, next_width), ladder_ints.dtype))
        scratch.append(pltpu.SemaphoreType.DMA((block_count, len(next_spots))))
    steps = block_count * len(spots)
    cost = pl.CostEstimate(
        flops=2 * steps * rows * depth * width, bytes_accessed=steps * 2 * depth * width, transcendentals=0
    )
    recv_picks = [picks_of(r, m) for r, m in zip(recvs, masks)]
    cfg = (parts, count, first_col, recv_picks, own_picks, rows, width, spots, next_width, next_spots, masking)
    return pl.pallas_call(
        functools.partial(send_kernel, cfg),
        in_specs=in_specs,
        out_specs=[IN_VMEM] * len(out_shape),
        scratch_shapes=scratch,
        out_shape=out_shape,
        cost_estimate=cost,
        compiler_params=pltpu.CompilerParams(vmem_limit_bytes=VMEM_LIMIT),
    )(*operands)


def finish_kernel(cfg, *refs):
    parts, rows, width, start, first_turn, want_update, want_squares, with_alias = cfg
    refs = list(refs)
    take = lambda n: [refs.pop(0) for _ in range(n)]
    own_ref, t_ref, occ_ref, vir_ref, occ_live_ref, vir_live_ref = take(6)
    recv_refs = take(parts)
    take(with_alias)
    (out_ref,) = take(1) if want_update else (None,)
    (sum_ref,) = take(1) if want_squares else (None,)
    block = pl.program_id(0)
    blocks, _, depth = t_ref.shape
    half = rows // 2
    tiles = width // LANES
    if first_turn:
        (column_ref,) = take(1)
        for r in range(0, rows, CODE_ROWS * 5):
            size = min(CODE_ROWS * 5, rows - r)
            row_index = lax.broadcasted_iota(jnp.int32, (size, rows), 0) + r
            col_index = lax.broadcasted_iota(jnp.int32, (size, rows), 1)
            occ = occ_ref[0:1, :]
            for h in range(1, blocks):
                occ = jnp.where(block == h, occ_ref[h : h + 1, :], occ)
            column = jnp.sum(jnp.where(row_index == col_index, occ, 0.0), axis=1, keepdims=True)
            column_ref[block, r : r + size, :] = jnp.broadcast_to(column, (size, LANES))
    else:
        column_ref = occ_ref
    block_id = lax.axis_index("irrep") * blocks + block
    occ_live = occ_live_ref[block_id]
    vir_live = vir_live_ref[block_id] - my_slot() * depth - start
    squares = jnp.zeros((CODE_ROWS, LANES), jnp.float32)
    row_index = lax.broadcasted_iota(jnp.int32, (half, LANES), 0)
    lane_index = lax.broadcasted_iota(jnp.int32, (half, LANES), 1)
    spans = [slice(0, half), slice(half, rows)]
    for c in range(parts):
        firsts = [c * width + t * LANES for t in range(tiles)]
        total = [tuple(own_ref[block, span, first : first + LANES] for span in spans) for first in firsts]
        total = unpack_add(total, recv_refs[c], blocks, block, rows, width)
        for t, first in enumerate(firsts):
            cols = slice(first, first + LANES)
            here = slice(start + first, start + first + LANES)
            vir = vir_ref[0:1, here]
            for h in range(1, blocks):
                vir = jnp.where(block == h, vir_ref[h : h + 1, here], vir)
            for part, span in enumerate(spans):
                keep = (row_index + part * half < occ_live) & (lane_index + first < vir_live)
                wide = t_ref[block, span, here].astype(jnp.float32)
                denominator = vir - column_ref[block, span, :]
                residual = jnp.where(keep, total[t][part] + denominator * wide, 0.0)
                if want_update:
                    out_ref[span, cols] = (wide - residual / (denominator + LEVEL_SHIFT)).astype(jnp.bfloat16)
                if want_squares:
                    squares += jnp.sum((residual * residual).reshape(-1, CODE_ROWS, LANES), axis=0)
    if want_squares:
        pair_count = jnp.full(squares.shape, occ_live * vir_live_ref[block_id], jnp.int32)
        sum_ref[...] = squares / pair_count.astype(jnp.float32)


def finish_call(t_masked, own, occ, vir_energy, live, width, start, recvs, updated, want_update, want_squares):
    block_count, rows, depth = t_masked.shape
    parts = len(recvs)
    both = parts * width
    first_turn = occ.ndim == 2
    operands = [own, t_masked, occ, vir_energy, *live] + [array for array, _ in recvs]
    in_specs = [IN_VMEM] * 4 + [IN_SMEM] * 2 + [IN_VMEM] * parts
    aliases = {}
    with_alias = int(want_update and updated is not None)
    if with_alias:
        in_specs.append(IN_HBM)
        operands.append(updated)
        aliases = {len(operands) - 1: 0}
    out_specs, out_shape = [], []
    if want_update:
        out_specs.append(pl.BlockSpec((None, rows, both), lambda h: (h, 0, start // both)))
        out_shape.append(jax.ShapeDtypeStruct((block_count, rows, depth), jnp.bfloat16))
    if want_squares:
        out_specs.append(pl.BlockSpec((None, CODE_ROWS, LANES), lambda h: (h, 0, 0)))
        out_shape.append(jax.ShapeDtypeStruct((block_count, CODE_ROWS, LANES), jnp.float32))
    if first_turn:
        out_specs.append(IN_VMEM)
        out_shape.append(jax.ShapeDtypeStruct((block_count, rows, LANES), jnp.float32))
    cfg = (parts, rows, width, start, first_turn, want_update, want_squares, with_alias)
    return pl.pallas_call(
        functools.partial(finish_kernel, cfg),
        grid=(block_count,),
        in_specs=in_specs,
        out_specs=out_specs,
        out_shape=out_shape,
        input_output_aliases=aliases,
        cost_estimate=pl.CostEstimate(
            flops=60 * block_count * rows * both, bytes_accessed=10 * block_count * rows * both, transcendentals=0
        ),
        compiler_params=pltpu.CompilerParams(dimension_semantics=("arbitrary",), vmem_limit_bytes=VMEM_LIMIT),
    )(*operands)


def job_order(turns, stages):
    def near(n):
        return (n, 0, True)

    def far(n):
        return (n, 0, False)

    def later(n, t=1):
        return (n, t, None)

    if stages == 3 and len(turns) == 4:
        a, b, c, d = turns
        jobs = [near(a), near(b), later(a), later(b), near(c), far(a), later(c), far(b), near(d)]
        return jobs + [later(a, 2), later(b, 2), later(d), far(c), far(d), later(c, 2), later(d, 2)]
    jobs = [near(turns[0])]
    for n in turns:
        jobs += [near(n + 1)] if n + 1 in turns else []
        jobs.append(later(n))
    return jobs + [far(n) for n in turns] + [later(n, t) for t in range(2, stages) for n in turns]


def body(order, *arrays):
    return residual_step(order, *arrays)


def residual_step(order, amplitudes, ladder_ints, hole_ints, occ_energy, vir_energy, occ_pairs, vir_pairs):
    _, _, cols_here = amplitudes.shape
    devices = lax.axis_size(GROUP)
    live = [occ_pairs, vir_pairs]

    def swap(packet, mask):
        return lax.ppermute(packet, GROUP, [(d, d ^ mask) for d in range(devices)])

    stages = len(order)
    plan = turn_plan(cols_here, order)
    turns = list(range(len(plan)))
    held = [[[] for _ in orders] for _, _, orders in plan]

    def having(turn, masks):
        return [[p for p in had if m[0] in p[1]] for had, m in zip(held[turn], masks)]

    calls = []
    for turn, t, near in job_order(turns, stages):
        orders = plan[turn][2]
        wanted = [patterns(o[2:] if t == 0 else o[t + 1 :]) for o in orders]
        if near:
            wanted = [[m | (1 << o[1]) for m in w] for o, w in zip(orders, wanted)]
        calls.append((turn, t, wanted, [[m | (1 << o[t]) for m in w] for o, w in zip(orders, wanted)]))
    spots = [
        (plan[turn][0], spots_of(plan[turn][0], plan[turn][1], masks, t == stages - 1)) for turn, t, _, masks in calls
    ] + [(0, None)]
    t_here, owns = amplitudes, {}
    pieces = open_call(ladder_ints, spots[0])
    for n, (turn, t, wanted, masks) in enumerate(calls):
        width, start, orders = plan[turn]
        parts = len(orders)
        own = (hole_ints, having(turn, [[0]] * parts)) if t == stages - 1 else None
        outs = send_call(
            t_here, ladder_ints, None if n else live, width, start, masks, having(turn, masks), own, pieces,
            spots[n + 1],
        )
        if own is not None:
            owns[turn] = outs[parts]
        if n == 0:
            t_here = outs[parts]
        if spots[n + 1][1]:
            pieces = outs[-1]
        for c, o in enumerate(orders):
            packet = outs[c]
            if t == stages - 1 and turn == turns[-1] - 1:
                packet = lax.optimization_barrier((packet, held[turns[-1]][0][-1][0]))[0]
            held[turn][c].append((swap(packet, 1 << o[t]), wanted[c]))
    updated, sums, occ = None, [], occ_energy
    for turn in turns:
        width, start, _ = plan[turn]

        def finish(want_update, want_squares):
            return finish_call(
                t_here, owns[turn], occ, vir_energy, live, width, start, [h[-1] for h in held[turn]], updated,
                want_update, want_squares,
            )

        if turn == turns[-1] and turn:
            (squares,) = finish(False, True)
            (updated,) = finish(True, False)
        else:
            updated, squares, *rest = finish(True, True)
            occ = rest[0] if rest else occ
        sums.append(squares)
    squares = jnp.sum(functools.reduce(jnp.add, sums), axis=(1, 2))
    squares = squares + swap(squares, 1 << order[0])
    across = []
    for mask in patterns(order[1:])[1:]:
        across.append(swap(squares, mask))
    residual_norm = jnp.sqrt(functools.reduce(jnp.add, [squares] + across) + EPSILON)
    return (updated, residual_norm)


def solution(mesh):
    in_specs = (
        P("irrep", None, ("occ", "vir")),
        P("irrep", ("occ", "vir"), None),
        P("irrep", None, None),
        P("irrep", None),
        P("irrep", ("occ", "vir")),
        P(),
        P(),
    )
    out_specs = (P("irrep", None, ("occ", "vir")), P("irrep"))
    order = stage_bits(mesh)
    return jax.shard_map(
        functools.partial(body, order), mesh=mesh, in_specs=in_specs, out_specs=out_specs, check_vma=False
    )
```
